32 devices in a mesh: section: 2 (over y), dp: 16 (over z, x, core).
Axes of the slice: x: 2, y: 2, z: 4, core: 2. Of those that a mesh axis runs over, the one named last changes fastest.
Arguments:
- inputs: bfloat16 [4, 16, 198, 768], P(None, 'dp'), may hold values from -6 to 6
- ln1_gain: float32 [2, 768], P('section'), may hold values from 0.1 to 1.9
- ln1_bias: float32 [2, 768], P('section'), may hold values from -3 to 3
- qkv_weight: bfloat16 [2, 768, 2304], P('section'), may hold values from -0.21875 to 0.21875
- qv_bias: float32 [2, 1536], P('section'), may hold values from -3 to 3
- proj_weight: bfloat16 [2, 768, 768], P('section'), may hold values from -0.625 to 0.625
- proj_bias: float32 [2, 768], P('section'), may hold values from -3 to 3
- ln2_gain: float32 [2, 768], P('section'), may hold values from 0.1 to 1.9
- ln2_bias: float32 [2, 768], P('section'), may hold values from -3 to 3
- fc1_weight: bfloat16 [2, 768, 3072], P('section'), may hold values from -0.21875 to 0.21875
- fc1_bias: float32 [2, 3072], P('section'), may hold values from -3 to 3
- fc2_weight: bfloat16 [2, 3072, 768], P('section'), may hold values from -0.15625 to 0.15625
- fc2_bias: float32 [2, 768], P('section'), may hold values from -3 to 3
- keep_masks: int32 [2, 2, 4, 16], P('section', None, None, 'dp'), may hold values 0 or 1
- cotangent: bfloat16 [4, 16, 198, 768], P(None, 'dp'), may hold values from -6 to 6
Outputs:
- layer_outputs: bfloat16 [2, 4, 16, 198, 768], P('section', None, 'dp')
- input_grads: bfloat16 [2, 4, 16, 198, 768], P('section', None, 'dp')
- grad_ln1_gain: float32 [2, 768], P('section')
- grad_ln1_bias: float32 [2, 768], P('section')
- grad_qkv_weight: float32 [2, 768, 2304], P('section')
- grad_qv_bias: float32 [2, 1536], P('section')
- grad_proj_weight: float32 [2, 768, 768], P('section')
- grad_proj_bias: float32 [2, 768], P('section')
- grad_ln2_gain: float32 [2, 768], P('section')
- grad_ln2_bias: float32 [2, 768], P('section')
- grad_fc1_weight: float32 [2, 768, 3072], P('section')
- grad_fc1_bias: float32 [2, 3072], P('section')
- grad_fc2_weight: float32 [2, 3072, 768], P('section')
- grad_fc2_bias: float32 [2, 768], P('section')
The draws below stay inside these ranges and needn't reach their ends.
Inputs may be any that keep to these rules, and one draw needn't show every extreme that they name: `keep_masks`: 1 keeps a branch for that image, 0 drops it.
All inputs are finite; a program needn't handle non-finite values. No bound on the sum of `keep_masks` on one device may be relied on, other than what follows from the above.
Results may differ from the reference program's by a relative error of at most 0.015.
Values may be sent and summed in bfloat16 or wider, within the bound.
A program may use at most 256 MiB of HBM per device.

```python
import jax
import jax.numpy as jnp
from jax import lax

D = 768
HEADS = 12
HEAD_DIM = 64
FF = 3072
SEQ = 198
MICRO = 4
LAYERS = 2
IMAGES = 16


def place_ends(array, own_key, low, high):
    place = [jax.random.randint(jax.random.fold_in(own_key, axis), (), 0, length) for axis, length in enumerate(array.shape)]
    longest = array.shape.index(max(array.shape))
    next_to = place[:longest] + [(place[longest] + 1) % array.shape[longest]] + place[longest + 1:]
    return array.at[tuple(place)].set(low).at[tuple(next_to)].set(high)


def steps_of(own_key, dims, pieces, least, top_value):
    loudness, own = 1.0, jax.random.fold_in(own_key, 6)
    for dim, parts in pieces:
        steps = jnp.exp(jax.random.uniform(jax.random.fold_in(own, dim), (parts,), jnp.float32, least / len(pieces), top_value / len(pieces)))
        loudness = loudness * jnp.repeat(steps, dims[dim] // parts).reshape([-1 if axis == dim else 1 for axis in range(len(dims))])
    return loudness


def normal_values(key, shape, deviation, reach, split=(), kind=jnp.bfloat16):
    loudness = steps_of(key, shape, split, -0.22, 0.18) if split else 1.0
    result = jax.random.normal(key, shape, jnp.float32) * deviation * loudness
    return jnp.minimum(jnp.maximum(result, -reach), reach).astype(kind)


def setup_inputs(seed: int = 0) -> dict:
    keys = jax.random.split(jax.random.key(seed), 16)
    return {
        "inputs": normal_values(keys[0], (MICRO, IMAGES, SEQ, D), 1.0, 6.0, ((1, 16),)),
        "ln1_gain": jnp.clip(1.0 + 0.18 * jax.random.normal(keys[1], (LAYERS, D), jnp.float32), 0.1, 1.9),
        "ln1_bias": normal_values(keys[2], (LAYERS, D), 0.5, 3.0, ((0, 2),), jnp.float32),
        "qkv_weight": normal_values(keys[3], (LAYERS, D, 3 * D), D ** -0.5, 0.21875, ((0, 2),)),
        "qv_bias": normal_values(keys[4], (LAYERS, 2 * D), 0.5, 3.0, ((0, 2),), jnp.float32),
        "proj_weight": normal_values(keys[5], (LAYERS, D, D), (D // 8) ** -0.5, 0.625, ((0, 2),)),
        "proj_bias": normal_values(keys[6], (LAYERS, D), 0.5, 3.0, ((0, 2),), jnp.float32),
        "ln2_gain": jnp.clip(1.0 + 0.18 * jax.random.normal(keys[7], (LAYERS, D), jnp.float32), 0.1, 1.9),
        "ln2_bias": normal_values(keys[8], (LAYERS, D), 0.5, 3.0, ((0, 2),), jnp.float32),
        "fc1_weight": normal_values(keys[9], (LAYERS, D, FF), D ** -0.5, 0.21875, ((0, 2),)),
        "fc1_bias": normal_values(keys[10], (LAYERS, FF), 0.5, 3.0, ((0, 2),), jnp.float32),
        "fc2_weight": normal_values(keys[11], (LAYERS, FF, D), (FF // 2) ** -0.5, 0.15625, ((0, 2),)),
        "fc2_bias": normal_values(keys[12], (LAYERS, D), 0.5, 3.0, ((0, 2),), jnp.float32),
        "keep_masks": place_ends((jax.random.randint(keys[13], (LAYERS, 2, MICRO, IMAGES), 0, 10) < 9).astype(jnp.int32), jax.random.fold_in(keys[13], 1), 0, 1),
        "cotangent": normal_values(keys[14], (MICRO, IMAGES, SEQ, D), 1.0, 6.0, ((1, 16),)),
    }


@jax.custom_vjp
def low(v):
    return lax.optimization_barrier(v.astype(jnp.bfloat16)).astype(jnp.float32)

@jax.custom_vjp
def low_back(v):
    return v

def low_keep(v):
    return (low(v), None)

def low_pass(kept, grad):
    return (grad,)

def back_keep(v):
    return (v, None)

def back_low(kept, grad):
    return (low(grad),)
low.defvjp(low_keep, low_pass)
low_back.defvjp(back_keep, back_low)
highest = lax.Precision.HIGHEST
epsilon = 1e-06
survive = 1.0 / 0.9

def norm_rows(v, gain, shift):
    mean_v = lax.optimization_barrier(jnp.mean(v, axis=-1, keepdims=True))
    centered = v - mean_v
    var = lax.optimization_barrier(jnp.mean(centered * centered, axis=-1, keepdims=True))
    return centered * lax.rsqrt(var + epsilon) * gain + shift

def layer(h, params, keeps):
    ln1_gain, ln1_bias, qkv_weight, qv_bias, proj_weight, proj_bias, ln2_gain, ln2_bias, fc1_weight, fc1_bias, fc2_weight, fc2_bias = params
    h = low_back(h)
    images = h.shape[0]
    keep_attn = (keeps[0] * survive)[:, None, None]
    keep_mlp = (keeps[1] * survive)[:, None, None]
    a = low(norm_rows(h, ln1_gain, ln1_bias))
    qkv = jnp.einsum('isd,de->ise', a, qkv_weight, precision=highest)
    query = low_back(low(qkv[..., :D] + qv_bias[:D])).reshape(images, SEQ, HEADS, HEAD_DIM)
    keyed = low_back(low(qkv[..., D:2 * D])).reshape(images, SEQ, HEADS, HEAD_DIM)
    value = low_back(low(qkv[..., 2 * D:] + qv_bias[D:])).reshape(images, SEQ, HEADS, HEAD_DIM)
    scores = low_back(jnp.einsum('ishd,ithd->ihst', query, keyed, precision=highest) * HEAD_DIM ** (-0.5))
    probs = jax.nn.softmax(scores, axis=-1)
    attended = jnp.einsum('ihst,ithd->ishd', low(probs), value, precision=highest)
    attended = low_back(low(attended)).reshape(images, SEQ, D)
    branch = low_back(jnp.einsum('isd,de->ise', attended, proj_weight, precision=highest) + proj_bias)
    x_mid = h + keep_attn * branch
    c = low(norm_rows(x_mid, ln2_gain, ln2_bias))
    u = low_back(jnp.einsum('isd,df->isf', c, fc1_weight, precision=highest) + fc1_bias)
    g = low(jax.nn.gelu(u, approximate=False))
    mlp_out = low_back(jnp.einsum('isf,fd->isd', g, fc2_weight, precision=highest) + fc2_bias)
    x_end = x_mid + keep_mlp * mlp_out
    return low(x_end)

def reference(inputs, ln1_gain, ln1_bias, qkv_weight, qv_bias, proj_weight, proj_bias, ln2_gain, ln2_bias, fc1_weight, fc1_bias, fc2_weight, fc2_bias, keep_masks, cotangent):
    params_all = tuple((p.astype(jnp.float32) for p in (ln1_gain, ln1_bias, qkv_weight, qv_bias, proj_weight, proj_bias, ln2_gain, ln2_bias, fc1_weight, fc1_bias, fc2_weight, fc2_bias)))
    keeps_all = jnp.transpose(keep_masks.astype(jnp.float32), (2, 0, 1, 3))
    start = tuple((jnp.zeros_like(p) for p in params_all))

    def one_batch(totals, slices):
        batch_in, batch_ct, batch_keep = slices
        hidden = batch_in.astype(jnp.float32)
        outs_list = []
        pulls = []
        for level in range(LAYERS):
            level_params = tuple((p[level] for p in params_all))

            def apply(hh, pp, kk=batch_keep[level]):
                return layer(hh, pp, kk)
            hidden, pull = jax.vjp(apply, hidden, level_params)
            outs_list.append(hidden)
            pulls.append(pull)
        grad = batch_ct.astype(jnp.float32)
        grads_in = [None] * LAYERS
        totals = list(totals)
        for level in reversed(range(LAYERS)):
            grad, grad_params = pulls[level](grad)
            grads_in[level] = grad
            totals = [t.at[level].add(gp) for t, gp in zip(totals, grad_params)]
        stacked_out = jnp.stack(outs_list).astype(jnp.bfloat16)
        stacked_in = jnp.stack(grads_in).astype(jnp.bfloat16)
        return (tuple(totals), (stacked_out, stacked_in))
    totals, (outs_seq, grads_seq) = lax.scan(one_batch, start, (inputs, cotangent, keeps_all))
    layer_outputs = jnp.transpose(outs_seq, (1, 0, 2, 3, 4))
    input_grads = jnp.transpose(grads_seq, (1, 0, 2, 3, 4))
    return (layer_outputs, input_grads, totals[0], totals[1], totals[2], totals[3], totals[4], totals[5], totals[6], totals[7], totals[8], totals[9], totals[10], totals[11])
```

```python
import functools
import math

import jax
import jax.numpy as jnp
from jax import lax
from jax.experimental import pallas as pl
from jax.experimental.pallas import tpu as pltpu
from jax.sharding import PartitionSpec as P

HEAD_DIM = 64


epsilon = 1e-06
survive = 1.0 / 0.9


def from_behind(value, axis, steps):
    count = lax.axis_size(axis)
    initial, last = (max(0, -steps), min(count, count - steps))
    return lax.ppermute(value, axis, [(source, source + steps) for source in range(initial, last)])


def as_sent(x):

    def short(part):
        return part.astype(jnp.bfloat16) if part.dtype == jnp.float32 else part

    return jax.tree.map(short, x)


def norm_parts(values, gain, shift):
    mean_v = jnp.mean(values, axis=-1, keepdims=True)
    centered = values - mean_v
    var = jnp.mean(centered * centered, axis=-1, keepdims=True)
    factor = lax.rsqrt(var + epsilon)
    normed = centered * factor
    return (normed * gain + shift, normed, factor)


def norm_back(grad_out, normed, factor, gain):
    scaled = grad_out * gain
    grad_in = factor * (
        scaled
        - jnp.mean(scaled, axis=-1, keepdims=True)
        - normed * jnp.mean(scaled * normed, axis=-1, keepdims=True)
    )
    return (grad_in, jnp.sum(grad_out * normed, axis=0), jnp.sum(grad_out, axis=0))


def gelu_slope(u):
    return 0.5 * (1.0 + lax.erf(u / math.sqrt(2.0))) + u * jnp.exp(-0.5 * u * u) / math.sqrt(
        2.0 * math.pi
    )


def run_forward(layer_in, weights, keeps):
    (
        gain_one,
        shift_one,
        w_qkv,
        bias_qv,
        w_proj,
        b_proj,
        gain_two,
        shift_two,
        w_up,
        b_up,
        w_down,
        b_down,
    ) = weights
    images, length, width = layer_in.shape
    heads = width // HEAD_DIM
    rows = images * length
    scale = HEAD_DIM ** (-0.5)
    keep_attn = jnp.repeat(keeps[0], length)[:, None]
    keep_mlp = jnp.repeat(keeps[1], length)[:, None]
    h_rows = layer_in.astype(jnp.float32).reshape(rows, width)
    a_val, normed_one, factor_one = norm_parts(h_rows, gain_one, shift_one)
    a_low = a_val.astype(jnp.bfloat16)
    qkv = jnp.dot(a_low, w_qkv, preferred_element_type=jnp.float32)
    query = (
        (qkv[:, :width] + bias_qv[:width])
        .astype(jnp.bfloat16)
        .reshape(images, length, heads, HEAD_DIM)
    )
    keyed = qkv[:, width : 2 * width].astype(jnp.bfloat16).reshape(images, length, heads, HEAD_DIM)
    value = (
        (qkv[:, 2 * width :] + bias_qv[width:])
        .astype(jnp.bfloat16)
        .reshape(images, length, heads, HEAD_DIM)
    )
    scores = jnp.einsum("ishd,ithd->ihst", query, keyed, preferred_element_type=jnp.float32) * scale
    top = jnp.max(scores, axis=-1, keepdims=True)
    expd = jnp.exp(scores - top)
    probs = expd / jnp.sum(expd, axis=-1, keepdims=True)
    probs_low = probs.astype(jnp.bfloat16)
    attended = jnp.einsum("ihst,ithd->ishd", probs_low, value, preferred_element_type=jnp.float32)
    attended_low = attended.astype(jnp.bfloat16).reshape(rows, width)
    branch = jnp.dot(attended_low, w_proj, preferred_element_type=jnp.float32) + b_proj
    x_mid = h_rows + keep_attn * branch
    c_val, normed_two, factor_two = norm_parts(x_mid, gain_two, shift_two)
    c_low = c_val.astype(jnp.bfloat16)
    u_val = jnp.dot(c_low, w_up, preferred_element_type=jnp.float32) + b_up
    g_low = jax.nn.gelu(u_val, approximate=False).astype(jnp.bfloat16)
    mlp_out = jnp.dot(g_low, w_down, preferred_element_type=jnp.float32) + b_down
    x_end = x_mid + keep_mlp * mlp_out
    result = x_end.astype(jnp.bfloat16).reshape(images, length, width)
    saved = (
        normed_one,
        factor_one,
        a_low,
        query,
        keyed,
        value,
        probs,
        probs_low,
        attended_low,
        normed_two,
        factor_two,
        c_low,
        u_val,
        g_low,
        keep_attn,
        keep_mlp,
    )
    return (result, saved)


def run_backward(layer_in, weights, keeps, upstream):
    (
        gain_one,
        shift_one,
        w_qkv,
        bias_qv,
        w_proj,
        b_proj,
        gain_two,
        shift_two,
        w_up,
        b_up,
        w_down,
        b_down,
    ) = weights
    images, length, width = layer_in.shape
    heads = width // HEAD_DIM
    rows = images * length
    scale = HEAD_DIM ** (-0.5)
    (
        normed_one,
        factor_one,
        a_low,
        query,
        keyed,
        value,
        probs,
        probs_low,
        attended_low,
        normed_two,
        factor_two,
        c_low,
        u_val,
        g_low,
        keep_attn,
        keep_mlp,
    ) = run_forward(layer_in, weights, keeps)[1]
    d_end = upstream.astype(jnp.float32).reshape(rows, width)
    d_mlp = (d_end * keep_mlp).astype(jnp.bfloat16)
    grad_down_bias = jnp.sum(d_mlp.astype(jnp.float32), axis=0)
    d_gel = jnp.dot(d_mlp, w_down.T, preferred_element_type=jnp.float32)
    d_up = (d_gel * gelu_slope(u_val)).astype(jnp.bfloat16)
    grad_up_bias = jnp.sum(d_up.astype(jnp.float32), axis=0)
    d_c = jnp.dot(d_up, w_up.T, preferred_element_type=jnp.float32)
    d_mid_norm, grad_gain_two, grad_shift_two = norm_back(d_c, normed_two, factor_two, gain_two)
    d_mid = d_end + d_mid_norm
    d_branch = (d_mid * keep_attn).astype(jnp.bfloat16)
    grad_proj_bias = jnp.sum(d_branch.astype(jnp.float32), axis=0)
    d_att = jnp.dot(d_branch, w_proj.T, preferred_element_type=jnp.float32)
    d_att = d_att.astype(jnp.bfloat16).reshape(images, length, heads, HEAD_DIM)
    d_probs = jnp.einsum("ishd,ithd->ihst", d_att, value, preferred_element_type=jnp.float32)
    d_value = jnp.einsum("ihst,ishd->ithd", probs_low, d_att, preferred_element_type=jnp.float32)
    d_scores = probs * (d_probs - jnp.sum(d_probs * probs, axis=-1, keepdims=True))
    d_scores = d_scores.astype(jnp.bfloat16)
    d_query = (
        jnp.einsum("ihst,ithd->ishd", d_scores, keyed, preferred_element_type=jnp.float32) * scale
    )
    d_keyed = (
        jnp.einsum("ihst,ishd->ithd", d_scores, query, preferred_element_type=jnp.float32) * scale
    )
    d_qkv = jnp.concatenate(
        [d_query.reshape(rows, width), d_keyed.reshape(rows, width), d_value.reshape(rows, width)],
        axis=1,
    ).astype(jnp.bfloat16)
    column_sums = jnp.sum(d_qkv.astype(jnp.float32), axis=0)
    grad_bias_qv = jnp.concatenate([column_sums[:width], column_sums[2 * width :]])
    d_a = jnp.dot(d_qkv, w_qkv.T, preferred_element_type=jnp.float32)
    d_in_norm, grad_gain_one, grad_shift_one = norm_back(d_a, normed_one, factor_one, gain_one)
    d_in = (d_mid + d_in_norm).astype(jnp.bfloat16).reshape(images, length, width)
    small = (
        grad_gain_one,
        grad_shift_one,
        grad_bias_qv,
        grad_proj_bias,
        grad_gain_two,
        grad_shift_two,
        grad_up_bias,
        grad_down_bias,
    )
    left = jnp.concatenate([a_low, attended_low, c_low, g_low], axis=1)
    right = jnp.concatenate([d_qkv, d_branch, d_up, d_mlp], axis=1)
    return (d_in, left, right, jnp.concatenate(small))


COLS = 256
SLOTS = 8
LAST = 7


def reduce_kernel(
    count,
    width,
    hidden,
    left_ref,
    right_ref,
    small_ref,
    qkv_ref,
    proj_ref,
    up_ref,
    down_ref,
    small_out,
    partial,
    give,
    give_x,
    give_z,
    take,
    take_x,
    take_z,
    whole,
    sent_core,
    sent_x,
    sent_z,
    spread_z,
    spread_x,
    spread_core,
    got_core,
    got_x,
    got_z,
    held_z,
    held_x,
    held_core,
    out_sem,
):
    line = count // 4
    per = width // COLS
    up_chunks = hidden // COLS
    first_proj, first_up = (3 * per, 4 * per)
    first_down = first_up + up_chunks
    chunks = first_down + per * (hidden // width)
    me = lax.axis_index("dp")
    core = lax.rem(me, 2)
    chip = me // 2
    across = lax.rem(chip, 2)
    along = chip // 2
    half = 2 * line

    def device(z, x, k):
        return {"dp": (z * 2 + x) * 2 + k}

    other_core = device(along, across, 1 - core)
    other_x = device(along, 1 - across, core)
    others_z = [device(lax.rem(along + i, line), across, core) for i in range(1, line)]

    barrier = pltpu.get_barrier_semaphore()
    for peer in [other_core, other_x] + others_z:
        pl.semaphore_signal(barrier, inc=1, device_id=peer, device_id_type=pl.DeviceIdType.MESH)
    pl.semaphore_wait(barrier, 1 + line)

    own_half = core * half
    own_quarter = own_half + across * line
    own_piece = own_quarter + along

    def remote(src, dst, send, recv, peer):
        return pltpu.make_async_remote_copy(
            src_ref=src,
            dst_ref=dst,
            send_sem=send,
            recv_sem=recv,
            device_id=peer,
            device_id_type=pl.DeviceIdType.MESH,
        )

    def to_core(s):
        return remote(give.at[s], take.at[s], sent_core.at[s], got_core.at[s], other_core)

    def to_x(s):
        return remote(give_x.at[s], take_x.at[s], sent_x.at[s], got_x.at[s], other_x)

    def to_z(s):
        return [
            remote(
                give_z.at[s, lax.rem(along + i, line)],
                take_z.at[s, i - 1],
                sent_z.at[s, i - 1],
                got_z.at[s, i - 1],
                others_z[i - 1],
            )
            for i in range(1, line)
        ]

    def back_z(s):
        piece = whole.at[s, own_piece]
        return [
            remote(
                piece, piece, spread_z.at[s, i - 1], held_z.at[s, i - 1], others_z[i - 1]
            )
            for i in range(1, line)
        ]

    def back_x(s):
        part = whole.at[s, pl.ds(own_quarter, line)]
        return remote(part, part, spread_x.at[s], held_x.at[s], other_x)

    def back_core(s):
        part = whole.at[s, pl.ds(own_half, half)]
        return remote(part, part, spread_core.at[s], held_core.at[s], other_core)

    def for_output(u, s, act):
        def go(ref, row, column):
            columns = pl.ds(pl.multiple_of(column * COLS, COLS), COLS)
            dst = ref.at[:, :, columns] if row is None else ref.at[row, :, :, columns]
            act(pltpu.make_async_copy(whole.at[s], dst, out_sem.at[s]))

        @pl.when(u < first_proj)
        def _():
            go(qkv_ref, None, u)

        @pl.when((u >= first_proj) & (u < first_up))
        def _():
            go(proj_ref, None, u - first_proj)

        @pl.when((u >= first_up) & (u < first_down))
        def _():
            go(up_ref, None, u - first_up)

        @pl.when((u >= first_down) & (u < chunks))
        def _():
            go(down_ref, (u - first_down) // per, lax.rem(u - first_down, per))

        @pl.when(u == chunks)
        def _():
            go(small_out, None, 0)

    def step(t, carry):
        def stage(delay):
            u = t - delay
            return u, lax.rem(u + SLOTS, SLOTS), (u >= 0) & (u <= chunks)

        u7, s7, on7 = stage(7)

        @pl.when(on7)
        def _():
            for_output(u7, s7, lambda copy: copy.wait())
            to_core(s7).wait_send()
            to_x(s7).wait_send()
            for copy in to_z(s7) + back_z(s7):
                copy.wait_send()
            back_x(s7).wait_send()
            back_core(s7).wait_send()

        u6, s6, on6 = stage(6)

        @pl.when(on6)
        def _():
            back_core(s6).wait_recv()
            for_output(u6, s6, lambda copy: copy.start())

        u5, s5, on5 = stage(5)

        @pl.when(on5)
        def _():
            back_x(s5).wait_recv()
            back_core(s5).start()

        u4, s4, on4 = stage(4)

        @pl.when(on4)
        def _():
            for copy in back_z(s4):
                copy.wait_recv()
            back_x(s4).start()

        u3, s3, on3 = stage(3)

        @pl.when(on3)
        def _():
            for copy in to_z(s3):
                copy.wait_recv()
            total = partial[s3, own_piece]
            for i in range(line - 1):
                total = total + take_z[s3, i].astype(jnp.float32)
            whole[s3, own_piece] = total.astype(jnp.bfloat16)
            for copy in back_z(s3):
                copy.start()

        u2, s2, on2 = stage(2)

        @pl.when(on2)
        def _():
            to_x(s2).wait_recv()
            quarter = pl.ds(own_quarter, line)
            total = partial[s2, quarter] + take_x[s2].astype(jnp.float32)
            partial[s2, quarter] = total
            give_z[s2] = total.astype(jnp.bfloat16)
            for copy in to_z(s2):
                copy.start()

        u1, s1, on1 = stage(1)

        @pl.when(on1)
        def _():
            to_core(s1).wait_recv()
            mine = pl.ds(own_half, half)
            partial[s1, mine] = partial[s1, mine] + take[s1].astype(jnp.float32)
            give_x[s1] = partial[s1, pl.ds(own_half + (1 - across) * line, line)].astype(
                jnp.bfloat16
            )
            to_x(s1).start()

        u0, s0, on0 = stage(0)

        @pl.when(on0)
        def _():
            @pl.when(u0 < chunks)
            def _():
                def reached(k):
                    return (u0 + chunks - k) // chunks

                block = reached(first_proj) + reached(first_up)
                for row in range(hidden // width):
                    block = block + reached(first_down + per * row)
                column = u0
                for row in range(1, hidden // width):
                    column = column - per * reached(first_down + per * row)
                rows = pl.ds(pl.multiple_of(block * width, width), width)
                columns = pl.ds(pl.multiple_of(column * COLS, COLS), COLS)
                product = lax.dot_general(
                    left_ref[:, rows],
                    right_ref[:, columns],
                    (((0,), (0,)), ((), ())),
                    preferred_element_type=jnp.float32,
                )
                partial[s0] = product.reshape(partial.shape[1:])

            @pl.when(u0 == chunks)
            def _():
                partial[s0] = small_ref[...]

            give[s0] = partial[s0, pl.ds((1 - core) * half, half)].astype(jnp.bfloat16)
            to_core(s0).start()

        return carry

    lax.fori_loop(0, chunks + 1 + LAST, step, 0)


def sum_weight_grads(lefts, rights, small, width):
    count = lax.axis_size("dp")
    hidden = rights.shape[1] - 5 * width
    piece = width // count
    if width % COLS or count % 4 or width % (16 * count) or small.size > width * COLS:
        return sum_weight_grads_plain(lefts, rights, small, width)
    line = count // 4
    tile = (count, piece, COLS)
    small_in = jnp.pad(small, (0, width * COLS - small.size)).reshape(tile)
    low, dma = (jnp.bfloat16, pltpu.SemaphoreType.DMA)
    anywhere = pl.BlockSpec(memory_space=pl.ANY)
    vmem = pl.BlockSpec(memory_space=pltpu.VMEM)
    outs = pl.pallas_call(
        functools.partial(reduce_kernel, count, width, hidden),
        out_shape=(
            jax.ShapeDtypeStruct((count, piece, 3 * width), low),
            jax.ShapeDtypeStruct((count, piece, width), low),
            jax.ShapeDtypeStruct((count, piece, hidden), low),
            jax.ShapeDtypeStruct((hidden // width, count, piece, width), low),
            jax.ShapeDtypeStruct(tile, low),
        ),
        in_specs=[vmem, vmem, vmem],
        out_specs=(anywhere,) * 5,
        scratch_shapes=[
            pltpu.VMEM((SLOTS, count, piece, COLS), jnp.float32),
            pltpu.VMEM((SLOTS, 2 * line, piece, COLS), low),
            pltpu.VMEM((SLOTS, line, piece, COLS), low),
            pltpu.VMEM((SLOTS, line, piece, COLS), low),
            pltpu.VMEM((SLOTS, 2 * line, piece, COLS), low),
            pltpu.VMEM((SLOTS, line, piece, COLS), low),
            pltpu.VMEM((SLOTS, line - 1, piece, COLS), low),
            pltpu.VMEM((SLOTS, count, piece, COLS), low),
            dma((SLOTS,)),
            dma((SLOTS,)),
            dma((SLOTS, line - 1)),
            dma((SLOTS, line - 1)),
            dma((SLOTS,)),
            dma((SLOTS,)),
            dma((SLOTS,)),
            dma((SLOTS,)),
            dma((SLOTS, line - 1)),
            dma((SLOTS, line - 1)),
            dma((SLOTS,)),
            dma((SLOTS,)),
            dma((SLOTS,)),
        ],
        compiler_params=pltpu.CompilerParams(
            collective_id=0, has_side_effects=True, vmem_limit_bytes=60 * 1024 * 1024
        ),
    )(lefts, rights, small_in)
    qkv, proj, up, down, small_sum = (out.astype(jnp.float32) for out in outs)
    return (
        qkv.reshape(width, 3 * width),
        proj.reshape(width, width),
        up.reshape(width, hidden),
        down.reshape(hidden, width),
        small_sum.reshape(-1)[: small.size],
    )


def sum_weight_grads_plain(lefts, rights, small, width):
    hidden = rights.shape[1] - 5 * width

    def product(l_start, l_size, r_start, r_size):
        return lax.dot_general(
            lefts[:, l_start : l_start + l_size],
            rights[:, r_start : r_start + r_size],
            (((0,), (0,)), ((), ())),
            preferred_element_type=jnp.float32,
        )

    totals = (
        product(0, width, 0, 3 * width),
        product(width, width, 3 * width, width),
        product(2 * width, width, 4 * width, hidden),
        product(3 * width, hidden, 4 * width + hidden, width),
        jnp.pad(small, (0, -small.size % lax.axis_size("dp"))),
    )
    totals = lax.psum_scatter(totals, "dp", scatter_dimension=0, tiled=True)
    whole = lax.all_gather(as_sent(totals), "dp", axis=0, tiled=True)
    whole = jax.tree.map(lambda part: part.astype(jnp.float32), whole)
    return whole[:4] + (whole[4][: small.size],)


def per_device(
    inputs,
    ln1_gain,
    ln1_bias,
    qkv_weight,
    qv_bias,
    proj_weight,
    proj_bias,
    ln2_gain,
    ln2_bias,
    fc1_weight,
    fc1_bias,
    fc2_weight,
    fc2_bias,
    keep_masks,
    cotangent,
):
    weights = tuple(
        (
            w[0]
            for w in (
                ln1_gain,
                ln1_bias,
                qkv_weight,
                qv_bias,
                proj_weight,
                proj_bias,
                ln2_gain,
                ln2_bias,
                fc1_weight,
                fc1_bias,
                fc2_weight,
                fc2_bias,
            )
        )
    )
    section_index = lax.axis_index("section")
    first = section_index == 0
    micro = inputs.shape[0]
    keep_scaled = keep_masks[0].astype(jnp.float32) * survive

    def keeps_for(index):
        clipped = jnp.clip(index, 0, micro - 1)
        return lax.dynamic_index_in_dim(keep_scaled, clipped, 1, keepdims=False)

    received = jnp.zeros_like(inputs[0])
    kept_inputs = []
    results = []
    for tick in range(micro + 1):
        own = inputs[min(tick, micro - 1)]
        layer_in = jnp.where(first, own, received)
        kept_inputs.append(layer_in)
        result = run_forward(layer_in, weights, keeps_for(tick - section_index))[0]
        results.append(result)
        if tick < micro:
            received = from_behind(result, "section", 1)
    layer_outputs = jnp.where(first, jnp.stack(results[:micro]), jnp.stack(results[1:]))[None]
    returned = jnp.zeros_like(inputs[0])
    grads_in = []
    lefts, rights = ([], [])
    small_total = None
    for tick in range(micro + 1):
        index = micro - tick - section_index
        valid = (index >= 0) & (index < micro)
        own = cotangent[max(micro - 1 - tick, 0)]
        upstream = jnp.where(first, returned, own)
        upstream = jnp.where(valid, upstream, jnp.zeros_like(upstream))
        d_in, left, right, small = run_backward(
            kept_inputs[micro - tick], weights, keeps_for(index), upstream
        )
        grads_in.append(d_in)
        if tick < micro:
            returned = from_behind(d_in, "section", -1)
        pad = -left.shape[0] % 16
        lefts.append(jnp.pad(left, ((0, pad), (0, 0))))
        rights.append(jnp.pad(right, ((0, pad), (0, 0))))
        small_total = small if small_total is None else small_total + small
    lefts = jnp.concatenate(lefts)
    rights = jnp.concatenate(rights)
    width = inputs.shape[-1]
    qkv, proj, up, down, small = sum_weight_grads(lefts, rights, small_total, width)
    hidden = up.shape[1]
    sizes = (width, width, 2 * width, width, width, width, hidden, width)
    starts = [sum(sizes[:i]) for i in range(len(sizes))]
    parts = [small[s : s + size] for s, size in zip(starts, sizes)]
    whole = (
        parts[0], parts[1], qkv, parts[2], proj, parts[3],
        parts[4], parts[5], up, parts[6], down, parts[7],
    )
    input_grads = jnp.where(
        first, jnp.stack(grads_in[1:][::-1]), jnp.stack(grads_in[:micro][::-1])
    )[None]
    return (
        layer_outputs,
        input_grads,
        whole[0][None],
        whole[1][None],
        whole[2][None],
        whole[3][None],
        whole[4][None],
        whole[5][None],
        whole[6][None],
        whole[7][None],
        whole[8][None],
        whole[9][None],
        whole[10][None],
        whole[11][None],
    )


def solution(mesh):
    in_specs = (
        P(None, "dp", None, None),
        P("section", None),
        P("section", None),
        P("section", None, None),
        P("section", None),
        P("section", None, None),
        P("section", None),
        P("section", None),
        P("section", None),
        P("section", None, None),
        P("section", None),
        P("section", None, None),
        P("section", None),
        P("section", None, None, "dp"),
        P(None, "dp", None, None),
    )
    out_specs = (
        P("section", None, "dp", None, None),
        P("section", None, "dp", None, None),
        P("section", None),
        P("section", None),
        P("section", None, None),
        P("section", None),
        P("section", None, None),
        P("section", None),
        P("section", None),
        P("section", None),
        P("section", None, None),
        P("section", None),
        P("section", None, None),
        P("section", None),
    )
    return jax.shard_map(
        per_device, mesh=mesh, in_specs=in_specs, out_specs=out_specs, check_vma=False
    )
```

```python
import functools
import math

import jax
import jax.numpy as jnp
from jax import lax
from jax.experimental import pallas as pl
from jax.experimental.pallas import tpu as pltpu
from jax.sharding import PartitionSpec as P

HEAD_DIM = 64


epsilon = 1e-06
survive = 1.0 / 0.9


def as_sent(x):

    def short(part):
        return part.astype(jnp.bfloat16) if part.dtype == jnp.float32 else part

    return jax.tree.map(short, x)


def meet(peer):
    barrier = pltpu.get_barrier_semaphore()
    pl.semaphore_signal(barrier, inc=1, device_id=peer, device_id_type=pl.DeviceIdType.MESH)
    pl.semaphore_wait(barrier, 1)


def norm_stats(values):
    centered = values - jnp.mean(values, axis=-1, keepdims=True)
    factor = lax.rsqrt(jnp.mean(centered * centered, axis=-1, keepdims=True) + epsilon)
    return (centered * factor, factor)


def dot_nn(a, b):
    return lax.dot_general(a, b, (((1,), (0,)), ((), ())), preferred_element_type=jnp.float32)


def dot_nt(a, b):
    return lax.dot_general(a, b, (((1,), (1,)), ((), ())), preferred_element_type=jnp.float32)


def dot_tn(a, b):
    return lax.dot_general(a, b, (((0,), (0,)), ((), ())), preferred_element_type=jnp.float32)


def fill_rows(dst_ref, src_ref):
    tokens, rows = src_ref.shape[-2], dst_ref.shape[-2]
    edge = tokens // 16 * 16
    dst_ref[0, edge:rows, :] = jnp.zeros((rows - edge, dst_ref.shape[-1]), dst_ref.dtype)
    dst_ref[0, 0:tokens, :] = src_ref[0, 0]


def head_masks(rows):
    lane = lax.broadcasted_iota(jnp.int32, (rows, 2 * HEAD_DIM), 1)
    return (lane < HEAD_DIM, lane >= HEAD_DIM)


def softmax_rows(query, keyed, tokens):
    scores = dot_nt(query, keyed)
    column = lax.broadcasted_iota(jnp.int32, scores.shape, 1)
    scores = jnp.where(column < tokens, scores, -1e30)
    expd = jnp.exp(scores - jnp.max(scores, axis=-1, keepdims=True))
    return expd / jnp.sum(expd, axis=-1, keepdims=True)


def forward_kernel(
    keeps_ref,
    in_ref,
    ln1_gain,
    ln1_bias,
    w_qkv,
    qv_bias,
    w_proj,
    b_proj,
    ln2_gain,
    ln2_bias,
    w_up,
    b_up,
    w_down,
    b_down,
    y_ref,
    held_ref,
    left_ref,
    qkv_ref,
    slope_ref,
    mid_ref,
    recv,
    send,
    send_sem,
    recv_sem,
):
    m = pl.program_id(0)
    micro = pl.num_programs(0)
    section = lax.axis_index("section")
    peer = {"section": 1 - section}
    tokens, width = y_ref.shape[1:]
    hidden = w_up.shape[1]
    rows = held_ref.shape[1]

    @pl.when(m == 0)
    def _():
        meet(peer)

    def copy_of(i):
        return pltpu.make_async_remote_copy(
            src_ref=send.at[i],
            dst_ref=recv.at[i],
            send_sem=send_sem.at[i],
            recv_sem=recv_sem.at[i],
            device_id=peer,
            device_id_type=pl.DeviceIdType.MESH,
        )

    @pl.when(section == 0)
    def _():
        fill_rows(held_ref, in_ref)

    @pl.when(section == 1)
    def _():
        copy_of(m).wait_recv()
        held_ref[0] = recv[m]

    h = held_ref[0].astype(jnp.float32)
    normed, _ = norm_stats(h)
    a_low = (normed * ln1_gain[...] + ln1_bias[...]).astype(jnp.bfloat16)
    left_ref[0, :, 0:width] = a_low
    for part in range(3):
        span = slice(part * width, (part + 1) * width)
        product = dot_nn(a_low, w_qkv[:, span])
        if part == 0:
            product = product + qv_bias[:, 0:width]
        if part == 2:
            product = product + qv_bias[:, width:]
        qkv_ref[0, :, span] = product.astype(jnp.bfloat16)

    masks = head_masks(rows)
    pair = 2 * HEAD_DIM
    for p in range(width // pair):
        at = [slice(part * width + p * pair, part * width + (p + 1) * pair) for part in range(3)]
        query, keyed, value = (qkv_ref[0, :, span] for span in at)
        query = query * jnp.asarray(HEAD_DIM**-0.5, jnp.bfloat16)
        joined = None
        for mask in masks:
            probs = softmax_rows(jnp.where(mask, query, jnp.zeros_like(query)), keyed, tokens)
            one = dot_nn(probs.astype(jnp.bfloat16), jnp.where(mask, value, jnp.zeros_like(value)))
            joined = one if joined is None else joined + one
        left_ref[0, :, width + p * pair : width + (p + 1) * pair] = joined.astype(jnp.bfloat16)

    branch = dot_nn(left_ref[0, :, width : 2 * width], w_proj[...]) + b_proj[...]
    x_mid = h + keeps_ref[0, m] * branch
    mid_ref[0] = x_mid
    normed, _ = norm_stats(x_mid)
    c_low = (normed * ln2_gain[...] + ln2_bias[...]).astype(jnp.bfloat16)
    left_ref[0, :, 2 * width : 3 * width] = c_low
    total = None
    for part in range(hidden // width):
        span = slice(part * width, (part + 1) * width)
        u = dot_nn(c_low, w_up[:, span]) + b_up[:, span]
        normal = 0.5 * (1.0 + lax.erf(u * math.sqrt(0.5)))
        slope_ref[0, :, span] = normal + u * jnp.exp(-0.5 * u * u) * (1.0 / math.sqrt(2.0 * math.pi))
        g_low = (u * normal).astype(jnp.bfloat16)
        left_ref[0, :, (3 + part) * width : (4 + part) * width] = g_low
        one = dot_nn(g_low, w_down[span, :])
        total = one if total is None else total + one
    y = (x_mid + keeps_ref[1, m] * (total + b_down[...])).astype(jnp.bfloat16)
    y_ref[0] = y[0:tokens]

    @pl.when(section == 0)
    def _():
        send[m] = y
        copy_of(m).start()

    @pl.when((section == 0) & (m == micro - 1))
    def _():
        for i in range(send.shape[0]):
            copy_of(i).wait_send()


def backward_kernel(
    keeps_ref,
    cot_ref,
    held_ref,
    qkv_ref,
    slope_ref,
    mid_ref,
    ln1_gain,
    w_qkv,
    w_proj,
    ln2_gain,
    w_up,
    w_down,
    d_in_ref,
    right_ref,
    small_ref,
    recv,
    send,
    upstream,
    d_heads,
    send_sem,
    recv_sem,
):
    j = pl.program_id(0)
    micro = pl.num_programs(0)
    m = micro - 1 - j
    section = lax.axis_index("section")
    peer = {"section": 1 - section}
    tokens, width = d_in_ref.shape[1:]
    hidden = w_up.shape[1]
    rows = held_ref.shape[1]
    pair = 2 * HEAD_DIM
    scale = HEAD_DIM**-0.5

    @pl.when(j == 0)
    def _():
        meet(peer)
        small_ref[...] = jnp.zeros_like(small_ref)

    def copy_of(i):
        return pltpu.make_async_remote_copy(
            src_ref=send.at[i],
            dst_ref=recv.at[i],
            send_sem=send_sem.at[i],
            recv_sem=recv_sem.at[i],
            device_id=peer,
            device_id_type=pl.DeviceIdType.MESH,
        )

    @pl.when(section == 1)
    def _():
        fill_rows(upstream, cot_ref)

    @pl.when(section == 0)
    def _():
        copy_of(j).wait_recv()
        upstream[0] = recv[j]

    def add_small(row, values):
        small_ref[row : row + 1, :] += jnp.sum(values, axis=0, keepdims=True)

    keep_attn, keep_mlp = (keeps_ref[0, m], keeps_ref[1, m])
    d_end = upstream[0].astype(jnp.float32)
    dm_low = (d_end * keep_mlp).astype(jnp.bfloat16)
    first_up = 4 * width
    right_ref[0, :, first_up + hidden : first_up + hidden + width] = dm_low
    parts = hidden // width
    add_small(7 + parts, dm_low.astype(jnp.float32))
    d_c = None
    for part in range(parts):
        span = slice(part * width, (part + 1) * width)
        d_gel = dot_nt(dm_low, w_down[span, :])
        du_low = (d_gel * slope_ref[0, :, span]).astype(jnp.bfloat16)
        right_ref[0, :, first_up + part * width : first_up + (part + 1) * width] = du_low
        add_small(7 + part, du_low.astype(jnp.float32))
        one = dot_nt(du_low, w_up[:, span])
        d_c = one if d_c is None else d_c + one

    def norm_grad(grad, normed, factor, gain, row):
        add_small(row, grad * normed)
        add_small(row + 1, grad)
        scaled = grad * gain
        return factor * (
            scaled
            - jnp.mean(scaled, axis=-1, keepdims=True)
            - normed * jnp.mean(scaled * normed, axis=-1, keepdims=True)
        )

    normed, factor = norm_stats(mid_ref[0])
    d_mid = d_end + norm_grad(d_c, normed, factor, ln2_gain[...], 5)
    dz_low = (d_mid * keep_attn).astype(jnp.bfloat16)
    right_ref[0, :, 3 * width : first_up] = dz_low
    add_small(4, dz_low.astype(jnp.float32))
    d_heads[...] = dot_nt(dz_low, w_proj[...]).astype(jnp.bfloat16)

    masks = head_masks(rows)
    for p in range(width // pair):
        at = [slice(part * width + p * pair, part * width + (p + 1) * pair) for part in range(3)]
        query, keyed, value = (qkv_ref[0, :, span] for span in at)
        d_out = d_heads[:, at[0]]
        grads = [None, None, None]
        for mask in masks:

            def only(x):
                return jnp.where(mask, x, jnp.zeros_like(x))

            query_one, d_one = only(query), only(d_out)
            probs = softmax_rows(query_one * jnp.asarray(scale, jnp.bfloat16), keyed, tokens)
            d_probs = dot_nt(d_one, value)
            inner = jnp.sum(d_probs * probs, axis=-1, keepdims=True)
            ds_low = (probs * (d_probs - inner)).astype(jnp.bfloat16)
            found = (
                dot_nn(ds_low, only(keyed)),
                dot_tn(ds_low, query_one),
                dot_tn(probs.astype(jnp.bfloat16), d_one),
            )
            grads = [f if g is None else g + f for g, f in zip(grads, found)]
        right_ref[0, :, at[0]] = (grads[0] * scale).astype(jnp.bfloat16)
        right_ref[0, :, at[1]] = (grads[1] * scale).astype(jnp.bfloat16)
        right_ref[0, :, at[2]] = grads[2].astype(jnp.bfloat16)

    add_small(2, right_ref[0, :, 0:width].astype(jnp.float32))
    add_small(3, right_ref[0, :, 2 * width : 3 * width].astype(jnp.float32))
    d_a = dot_nt(right_ref[0, :, 0 : 3 * width], w_qkv[...])
    normed, factor = norm_stats(held_ref[0].astype(jnp.float32))
    d_in = d_mid + norm_grad(d_a, normed, factor, ln1_gain[...], 0)
    d_low = d_in.astype(jnp.bfloat16)
    d_in_ref[0] = d_low[0:tokens]

    @pl.when(section == 1)
    def _():
        send[j] = d_low
        copy_of(j).start()

    @pl.when((section == 1) & (j == micro - 1))
    def _():
        for i in range(send.shape[0]):
            copy_of(i).wait_send()


def run_layers(inputs, cotangent, weights, keeps):
    (
        gain_one, shift_one, w_qkv, bias_qv, w_proj, b_proj,
        gain_two, shift_two, w_up, b_up, w_down, b_down,
    ) = (w.reshape(1, -1) if w.ndim == 1 else w for w in weights)
    micro, _, tokens, width = inputs.shape
    hidden = w_up.shape[1]
    rows = tokens + -tokens % 16
    low, dma = (jnp.bfloat16, pltpu.SemaphoreType.DMA)

    def fixed(x):
        return pl.BlockSpec(x.shape, lambda i: (0,) * x.ndim, pipeline_mode=pl.Buffered(1))

    def per_step(order, *dims):
        return pl.BlockSpec((1,) + dims, lambda i: (order(i),) + (0,) * len(dims))

    def ahead(i):
        return i

    def back(i):
        return micro - 1 - i

    def params(which):
        return pltpu.CompilerParams(
            collective_id=which,
            has_side_effects=True,
            dimension_semantics=("arbitrary",),
            vmem_limit_bytes=60 * 1024 * 1024,
        )

    smem = pl.BlockSpec(memory_space=pltpu.SMEM)
    consts = (
        gain_one, shift_one, w_qkv, bias_qv, w_proj, b_proj,
        gain_two, shift_two, w_up, b_up, w_down, b_down,
    )
    lefts_width = 3 * width + hidden
    rights_width = 5 * width + hidden
    outputs, held, lefts, qkv, slope, mid = pl.pallas_call(
        forward_kernel,
        grid=(micro,),
        out_shape=(
            jax.ShapeDtypeStruct((micro, tokens, width), low),
            jax.ShapeDtypeStruct((micro, rows, width), low),
            jax.ShapeDtypeStruct((micro, rows, lefts_width), low),
            jax.ShapeDtypeStruct((micro, rows, 3 * width), low),
            jax.ShapeDtypeStruct((micro, rows, hidden), jnp.float32),
            jax.ShapeDtypeStruct((micro, rows, width), jnp.float32),
        ),
        in_specs=[smem, per_step(ahead, 1, tokens, width)] + [fixed(x) for x in consts],
        out_specs=(
            per_step(ahead, tokens, width),
            per_step(ahead, rows, width),
            per_step(ahead, rows, lefts_width),
            per_step(ahead, rows, 3 * width),
            per_step(ahead, rows, hidden),
            per_step(ahead, rows, width),
        ),
        scratch_shapes=[
            pltpu.VMEM((micro, rows, width), low),
            pltpu.VMEM((micro, rows, width), low),
            dma((micro,)),
            dma((micro,)),
        ],
        compiler_params=params(1),
    )(keeps, inputs, *consts)
    small_rows = 8 + hidden // width
    small_rows += -small_rows % 8
    consts = (gain_one, w_qkv, w_proj, gain_two, w_up, w_down)
    d_inputs, rights, small = pl.pallas_call(
        backward_kernel,
        grid=(micro,),
        out_shape=(
            jax.ShapeDtypeStruct((micro, tokens, width), low),
            jax.ShapeDtypeStruct((micro, rows, rights_width), low),
            jax.ShapeDtypeStruct((small_rows, width), jnp.float32),
        ),
        in_specs=[
            smem,
            per_step(back, 1, tokens, width),
            per_step(back, rows, width),
            per_step(back, rows, 3 * width),
            per_step(back, rows, hidden),
            per_step(back, rows, width),
        ]
        + [fixed(x) for x in consts],
        out_specs=(
            per_step(back, tokens, width),
            per_step(back, rows, rights_width),
            pl.BlockSpec((small_rows, width), lambda i: (0, 0)),
        ),
        scratch_shapes=[
            pltpu.VMEM((micro, rows, width), low),
            pltpu.VMEM((micro, rows, width), low),
            pltpu.VMEM((1, rows, width), low),
            pltpu.VMEM((rows, width), low),
            dma((micro,)),
            dma((micro,)),
        ],
        compiler_params=params(2),
    )(keeps, cotangent, held, qkv, slope, mid, *consts)
    return (
        outputs,
        d_inputs,
        lefts.reshape(micro * rows, lefts_width),
        rights.reshape(micro * rows, rights_width),
        small,
    )


COLS = 256
SLOTS = 8
LAST = 7


def reduce_kernel(
    count,
    width,
    hidden,
    left_ref,
    right_ref,
    small_ref,
    qkv_ref,
    proj_ref,
    up_ref,
    down_ref,
    small_out,
    partial,
    give,
    give_x,
    give_z,
    take,
    take_x,
    take_z,
    whole,
    sent_core,
    sent_x,
    sent_z,
    spread_z,
    spread_x,
    spread_core,
    got_core,
    got_x,
    got_z,
    held_z,
    held_x,
    held_core,
    out_sem,
):
    line = count // 4
    per = width // COLS
    up_chunks = hidden // COLS
    first_proj, first_up = (3 * per, 4 * per)
    first_down = first_up + up_chunks
    chunks = first_down + per * (hidden // width)
    me = lax.axis_index("dp")
    core = lax.rem(me, 2)
    chip = me // 2
    across = lax.rem(chip, 2)
    along = chip // 2
    half = 2 * line

    def device(z, x, k):
        return {"dp": (z * 2 + x) * 2 + k}

    other_core = device(along, across, 1 - core)
    other_x = device(along, 1 - across, core)
    others_z = [device(lax.rem(along + i, line), across, core) for i in range(1, line)]

    barrier = pltpu.get_barrier_semaphore()
    for peer in [other_core, other_x] + others_z:
        pl.semaphore_signal(barrier, inc=1, device_id=peer, device_id_type=pl.DeviceIdType.MESH)
    pl.semaphore_wait(barrier, 1 + line)

    own_half = core * half
    own_quarter = own_half + across * line
    own_piece = own_quarter + along

    def remote(src, dst, send, recv, peer):
        return pltpu.make_async_remote_copy(
            src_ref=src,
            dst_ref=dst,
            send_sem=send,
            recv_sem=recv,
            device_id=peer,
            device_id_type=pl.DeviceIdType.MESH,
        )

    def to_core(s):
        return remote(give.at[s], take.at[s], sent_core.at[s], got_core.at[s], other_core)

    def to_x(s):
        return remote(give_x.at[s], take_x.at[s], sent_x.at[s], got_x.at[s], other_x)

    def to_z(s):
        return [
            remote(
                give_z.at[s, lax.rem(along + i, line)],
                take_z.at[s, i - 1],
                sent_z.at[s, i - 1],
                got_z.at[s, i - 1],
                others_z[i - 1],
            )
            for i in range(1, line)
        ]

    def back_z(s):
        piece = whole.at[s, own_piece]
        return [
            remote(
                piece, piece, spread_z.at[s, i - 1], held_z.at[s, i - 1], others_z[i - 1]
            )
            for i in range(1, line)
        ]

    def back_x(s):
        part = whole.at[s, pl.ds(own_quarter, line)]
        return remote(part, part, spread_x.at[s], held_x.at[s], other_x)

    def back_core(s):
        part = whole.at[s, pl.ds(own_half, half)]
        return remote(part, part, spread_core.at[s], held_core.at[s], other_core)

    def for_output(u, s, act):
        def go(ref, row, column):
            columns = pl.ds(pl.multiple_of(column * COLS, COLS), COLS)
            dst = ref.at[:, :, columns] if row is None else ref.at[row, :, :, columns]
            act(pltpu.make_async_copy(whole.at[s], dst, out_sem.at[s]))

        @pl.when(u < first_proj)
        def _():
            go(qkv_ref, None, u)

        @pl.when((u >= first_proj) & (u < first_up))
        def _():
            go(proj_ref, None, u - first_proj)

        @pl.when((u >= first_up) & (u < first_down))
        def _():
            go(up_ref, None, u - first_up)

        @pl.when((u >= first_down) & (u < chunks))
        def _():
            go(down_ref, (u - first_down) // per, lax.rem(u - first_down, per))

        @pl.when(u == chunks)
        def _():
            go(small_out, None, 0)

    def step(t, carry):
        def stage(delay):
            u = t - delay
            return u, lax.rem(u + SLOTS, SLOTS), (u >= 0) & (u <= chunks)

        u7, s7, on7 = stage(7)

        @pl.when(on7)
        def _():
            for_output(u7, s7, lambda copy: copy.wait())
            to_core(s7).wait_send()
            to_x(s7).wait_send()
            for copy in to_z(s7) + back_z(s7):
                copy.wait_send()
            back_x(s7).wait_send()
            back_core(s7).wait_send()

        u6, s6, on6 = stage(6)

        @pl.when(on6)
        def _():
            back_core(s6).wait_recv()
            for_output(u6, s6, lambda copy: copy.start())

        u5, s5, on5 = stage(5)

        @pl.when(on5)
        def _():
            back_x(s5).wait_recv()
            back_core(s5).start()

        u4, s4, on4 = stage(4)

        @pl.when(on4)
        def _():
            for copy in back_z(s4):
                copy.wait_recv()
            back_x(s4).start()

        u3, s3, on3 = stage(3)

        @pl.when(on3)
        def _():
            for copy in to_z(s3):
                copy.wait_recv()
            total = partial[s3, own_piece]
            for i in range(line - 1):
                total = total + take_z[s3, i].astype(jnp.float32)
            whole[s3, own_piece] = total.astype(jnp.bfloat16)
            for copy in back_z(s3):
                copy.start()

        u2, s2, on2 = stage(2)

        @pl.when(on2)
        def _():
            to_x(s2).wait_recv()
            quarter = pl.ds(own_quarter, line)
            total = partial[s2, quarter] + take_x[s2].astype(jnp.float32)
            partial[s2, quarter] = total
            give_z[s2] = total.astype(jnp.bfloat16)
            for copy in to_z(s2):
                copy.start()

        u1, s1, on1 = stage(1)

        @pl.when(on1)
        def _():
            to_core(s1).wait_recv()
            mine = pl.ds(own_half, half)
            partial[s1, mine] = partial[s1, mine] + take[s1].astype(jnp.float32)
            give_x[s1] = partial[s1, pl.ds(own_half + (1 - across) * line, line)].astype(
                jnp.bfloat16
            )
            to_x(s1).start()

        u0, s0, on0 = stage(0)

        @pl.when(on0)
        def _():
            @pl.when(u0 < chunks)
            def _():
                def reached(k):
                    return (u0 + chunks - k) // chunks

                block = reached(first_proj) + reached(first_up)
                for row in range(hidden // width):
                    block = block + reached(first_down + per * row)
                column = u0
                for row in range(1, hidden // width):
                    column = column - per * reached(first_down + per * row)
                rows = pl.ds(pl.multiple_of(block * width, width), width)
                columns = pl.ds(pl.multiple_of(column * COLS, COLS), COLS)
                product = lax.dot_general(
                    left_ref[:, rows],
                    right_ref[:, columns],
                    (((0,), (0,)), ((), ())),
                    preferred_element_type=jnp.float32,
                )
                partial[s0] = product.reshape(partial.shape[1:])

            @pl.when(u0 == chunks)
            def _():
                partial[s0] = jnp.zeros(partial.shape[1:], jnp.float32)
                partial[s0, 0] = small_ref[...]

            give[s0] = partial[s0, pl.ds((1 - core) * half, half)].astype(jnp.bfloat16)
            to_core(s0).start()

        return carry

    lax.fori_loop(0, chunks + 1 + LAST, step, 0)


def sum_weight_grads(lefts, rights, small, width):
    count = lax.axis_size("dp")
    small = small.reshape(-1)
    hidden = rights.shape[1] - 5 * width
    piece = width // count
    if width % COLS or count % 4 or width % (16 * count) or small.size > piece * COLS:
        return sum_weight_grads_plain(lefts, rights, small, width)
    line = count // 4
    tile = (count, piece, COLS)
    small_in = jnp.pad(small, (0, piece * COLS - small.size)).reshape(piece, COLS)
    low, dma = (jnp.bfloat16, pltpu.SemaphoreType.DMA)
    anywhere = pl.BlockSpec(memory_space=pl.ANY)
    vmem = pl.BlockSpec(memory_space=pltpu.VMEM)
    outs = pl.pallas_call(
        functools.partial(reduce_kernel, count, width, hidden),
        out_shape=(
            jax.ShapeDtypeStruct((count, piece, 3 * width), low),
            jax.ShapeDtypeStruct((count, piece, width), low),
            jax.ShapeDtypeStruct((count, piece, hidden), low),
            jax.ShapeDtypeStruct((hidden // width, count, piece, width), low),
            jax.ShapeDtypeStruct(tile, low),
        ),
        in_specs=[vmem, vmem, vmem],
        out_specs=(anywhere,) * 5,
        scratch_shapes=[
            pltpu.VMEM((SLOTS, count, piece, COLS), jnp.float32),
            pltpu.VMEM((SLOTS, 2 * line, piece, COLS), low),
            pltpu.VMEM((SLOTS, line, piece, COLS), low),
            pltpu.VMEM((SLOTS, line, piece, COLS), low),
            pltpu.VMEM((SLOTS, 2 * line, piece, COLS), low),
            pltpu.VMEM((SLOTS, line, piece, COLS), low),
            pltpu.VMEM((SLOTS, line - 1, piece, COLS), low),
            pltpu.VMEM((SLOTS, count, piece, COLS), low),
            dma((SLOTS,)),
            dma((SLOTS,)),
            dma((SLOTS, line - 1)),
            dma((SLOTS, line - 1)),
            dma((SLOTS,)),
            dma((SLOTS,)),
            dma((SLOTS,)),
            dma((SLOTS,)),
            dma((SLOTS, line - 1)),
            dma((SLOTS, line - 1)),
            dma((SLOTS,)),
            dma((SLOTS,)),
            dma((SLOTS,)),
        ],
        compiler_params=pltpu.CompilerParams(
            collective_id=0, has_side_effects=True, vmem_limit_bytes=60 * 1024 * 1024
        ),
    )(lefts, rights, small_in)
    qkv, proj, up, down, small_sum = (out.astype(jnp.float32) for out in outs)
    return (
        qkv.reshape(width, 3 * width),
        proj.reshape(width, width),
        up.reshape(width, hidden),
        down.reshape(hidden, width),
        small_sum[0].reshape(-1)[: small.size],
    )


def sum_weight_grads_plain(lefts, rights, small, width):
    hidden = rights.shape[1] - 5 * width

    def product(l_start, l_size, r_start, r_size):
        return lax.dot_general(
            lefts[:, l_start : l_start + l_size],
            rights[:, r_start : r_start + r_size],
            (((0,), (0,)), ((), ())),
            preferred_element_type=jnp.float32,
        )

    totals = (
        product(0, width, 0, 3 * width),
        product(width, width, 3 * width, width),
        product(2 * width, width, 4 * width, hidden),
        product(3 * width, hidden, 4 * width + hidden, width),
        jnp.pad(small, (0, -small.size % lax.axis_size("dp"))),
    )
    totals = lax.psum_scatter(totals, "dp", scatter_dimension=0, tiled=True)
    whole = lax.all_gather(as_sent(totals), "dp", axis=0, tiled=True)
    whole = jax.tree.map(lambda part: part.astype(jnp.float32), whole)
    return whole[:4] + (whole[4][: small.size],)


def per_device(
    inputs,
    ln1_gain,
    ln1_bias,
    qkv_weight,
    qv_bias,
    proj_weight,
    proj_bias,
    ln2_gain,
    ln2_bias,
    fc1_weight,
    fc1_bias,
    fc2_weight,
    fc2_bias,
    keep_masks,
    cotangent,
):
    weights = tuple(
        (
            w[0]
            for w in (
                ln1_gain,
                ln1_bias,
                qkv_weight,
                qv_bias,
                proj_weight,
                proj_bias,
                ln2_gain,
                ln2_bias,
                fc1_weight,
                fc1_bias,
                fc2_weight,
                fc2_bias,
            )
        )
    )
    keeps = keep_masks[0, :, :, 0].astype(jnp.float32) * survive
    outputs, d_inputs, lefts, rights, small = run_layers(inputs, cotangent, weights, keeps)
    layer_outputs = outputs[None, :, None]
    input_grads = d_inputs[None, :, None]
    width = inputs.shape[-1]
    qkv, proj, up, down, small = sum_weight_grads(lefts, rights, small, width)
    hidden = up.shape[1]
    sizes = (width, width, 2 * width, width, width, width, hidden, width)
    starts = [sum(sizes[:i]) for i in range(len(sizes))]
    parts = [small[s : s + size] for s, size in zip(starts, sizes)]
    whole = (
        parts[0], parts[1], qkv, parts[2], proj, parts[3],
        parts[4], parts[5], up, parts[6], down, parts[7],
    )
    return (
        layer_outputs,
        input_grads,
        whole[0][None],
        whole[1][None],
        whole[2][None],
        whole[3][None],
        whole[4][None],
        whole[5][None],
        whole[6][None],
        whole[7][None],
        whole[8][None],
        whole[9][None],
        whole[10][None],
        whole[11][None],
    )


def solution(mesh):
    in_specs = (
        P(None, "dp", None, None),
        P("section", None),
        P("section", None),
        P("section", None, None),
        P("section", None),
        P("section", None, None),
        P("section", None),
        P("section", None),
        P("section", None),
        P("section", None, None),
        P("section", None),
        P("section", None, None),
        P("section", None),
        P("section", None, None, "dp"),
        P(None, "dp", None, None),
    )
    out_specs = (
        P("section", None, "dp", None, None),
        P("section", None, "dp", None, None),
        P("section", None),
        P("section", None),
        P("section", None, None),
        P("section", None),
        P("section", None, None),
        P("section", None),
        P("section", None),
        P("section", None),
        P("section", None, None),
        P("section", None),
        P("section", None, None),
        P("section", None),
    )
    return jax.shard_map(
        per_device, mesh=mesh, in_specs=in_specs, out_specs=out_specs, check_vma=False
    )
```

```python
import functools
import math

import jax
import jax.numpy as jnp
from jax import lax
from jax.experimental import pallas as pl
from jax.experimental.pallas import tpu as pltpu
from jax.sharding import PartitionSpec as P

HEAD_DIM = 64


epsilon = 1e-06
survive = 1.0 / 0.9


def as_sent(x):

    def short(part):
        return part.astype(jnp.bfloat16) if part.dtype == jnp.float32 else part

    return jax.tree.map(short, x)


def meet(peer):
    barrier = pltpu.get_barrier_semaphore()
    pl.semaphore_signal(barrier, inc=1, device_id=peer, device_id_type=pl.DeviceIdType.MESH)
    pl.semaphore_wait(barrier, 1)


def kept(keeps_ref, branch, m):
    return keeps_ref[branch, m].astype(jnp.float32) * survive


def norm_stats(values):
    centered = values - jnp.mean(values, axis=-1, keepdims=True)
    factor = lax.rsqrt(jnp.mean(centered * centered, axis=-1, keepdims=True) + epsilon)
    return (centered * factor, factor)


def loader(first, sems, pairs):
    copies = {
        name: pltpu.make_async_copy(src, dst, sems.at[i])
        for i, (name, (src, dst)) in enumerate(pairs.items())
    }

    @pl.when(first)
    def _():
        for copy in copies.values():
            copy.start()

    def need(name):
        @pl.when(first)
        def _():
            copies[name].wait()

    return need


def dot_nn(a, b):
    return lax.dot_general(a, b, (((1,), (0,)), ((), ())), preferred_element_type=jnp.float32)


def dot_nt(a, b):
    return lax.dot_general(a, b, (((1,), (1,)), ((), ())), preferred_element_type=jnp.float32)


def dot_tn(a, b):
    return lax.dot_general(a, b, (((0,), (0,)), ((), ())), preferred_element_type=jnp.float32)


def fill_rows(dst_ref, src_ref):
    tokens, rows = src_ref.shape[-2], dst_ref.shape[-2]
    edge = tokens // 16 * 16
    dst_ref[0, edge:rows, :] = jnp.zeros((rows - edge, dst_ref.shape[-1]), dst_ref.dtype)
    dst_ref[0, 0:tokens, :] = src_ref[0, 0]


def head_masks(rows):
    lane = lax.broadcasted_iota(jnp.int32, (rows, 2 * HEAD_DIM), 1)
    return (lane < HEAD_DIM, lane >= HEAD_DIM)


def softmax_rows(query, keyed, tokens):
    scores = dot_nt(query, keyed)
    column = lax.broadcasted_iota(jnp.int32, scores.shape, 1)
    scores = jnp.where(column < tokens, scores, -1e30)
    expd = jnp.exp(scores - jnp.max(scores, axis=-1, keepdims=True))
    return expd / jnp.sum(expd, axis=-1, keepdims=True)


def forward_kernel(
    keeps_ref,
    in_ref,
    ln1_gain,
    ln1_bias,
    w_qkv,
    qv_bias,
    w_proj,
    b_proj,
    ln2_gain,
    ln2_bias,
    w_up,
    b_up,
    w_down,
    b_down,
    y_ref,
    held_ref,
    left_ref,
    qkv_ref,
    slope_ref,
    mid_ref,
    recv,
    send,
    send_sem,
    recv_sem,
    v_qkv,
    v_proj,
    v_up,
    v_down,
    load_sem,
):
    m = pl.program_id(0)
    micro = pl.num_programs(0)
    need = loader(
        m == 0,
        load_sem,
        {"qkv": (w_qkv, v_qkv), "proj": (w_proj, v_proj), "up": (w_up, v_up), "down": (w_down, v_down)},
    )
    section = lax.axis_index("section")
    peer = {"section": 1 - section}
    tokens, width = y_ref.shape[1:]
    hidden = w_up.shape[1]
    rows = held_ref.shape[1]

    @pl.when(m == 0)
    def _():
        meet(peer)

    def copy_of(i):
        return pltpu.make_async_remote_copy(
            src_ref=send.at[i],
            dst_ref=recv.at[i],
            send_sem=send_sem.at[i],
            recv_sem=recv_sem.at[i],
            device_id=peer,
            device_id_type=pl.DeviceIdType.MESH,
        )

    @pl.when(section == 0)
    def _():
        fill_rows(held_ref, in_ref)

    @pl.when(section == 1)
    def _():
        copy_of(m).wait_recv()
        held_ref[0] = recv[m]

    h = held_ref[0].astype(jnp.float32)
    normed, _ = norm_stats(h)
    a_low = (normed * ln1_gain[...] + ln1_bias[...]).astype(jnp.bfloat16)
    left_ref[0, :, 0:width] = a_low
    need("qkv")
    for part in range(3):
        span = slice(part * width, (part + 1) * width)
        product = dot_nn(a_low, v_qkv[:, span])
        if part == 0:
            product = product + qv_bias[:, 0:width]
        if part == 2:
            product = product + qv_bias[:, width:]
        qkv_ref[0, :, span] = product.astype(jnp.bfloat16)

    masks = head_masks(rows)
    pair = 2 * HEAD_DIM
    for p in range(width // pair):
        at = [slice(part * width + p * pair, part * width + (p + 1) * pair) for part in range(3)]
        query, keyed, value = (qkv_ref[0, :, span] for span in at)
        query = query * jnp.asarray(HEAD_DIM**-0.5, jnp.bfloat16)
        joined = None
        for mask in masks:
            probs = softmax_rows(jnp.where(mask, query, jnp.zeros_like(query)), keyed, tokens)
            one = dot_nn(probs.astype(jnp.bfloat16), jnp.where(mask, value, jnp.zeros_like(value)))
            joined = one if joined is None else joined + one
        left_ref[0, :, width + p * pair : width + (p + 1) * pair] = joined.astype(jnp.bfloat16)

    need("proj")
    branch = dot_nn(left_ref[0, :, width : 2 * width], v_proj[...]) + b_proj[...]
    x_mid = h + kept(keeps_ref, 0, m) * branch
    mid_ref[0] = x_mid
    normed, _ = norm_stats(x_mid)
    c_low = (normed * ln2_gain[...] + ln2_bias[...]).astype(jnp.bfloat16)
    left_ref[0, :, 2 * width : 3 * width] = c_low
    need("up")
    need("down")
    total = None
    for part in range(hidden // width):
        span = slice(part * width, (part + 1) * width)
        u = dot_nn(c_low, v_up[:, span]) + b_up[:, span]
        normal = 0.5 * (1.0 + lax.erf(u * math.sqrt(0.5)))
        slope_ref[0, :, span] = normal + u * jnp.exp(-0.5 * u * u) * (1.0 / math.sqrt(2.0 * math.pi))
        g_low = (u * normal).astype(jnp.bfloat16)
        left_ref[0, :, (3 + part) * width : (4 + part) * width] = g_low
        one = dot_nn(g_low, v_down[span, :])
        total = one if total is None else total + one
    y = (x_mid + kept(keeps_ref, 1, m) * (total + b_down[...])).astype(jnp.bfloat16)
    y_ref[0] = y[0:tokens]

    @pl.when(section == 0)
    def _():
        send[m] = y
        copy_of(m).start()

    @pl.when((section == 0) & (m == micro - 1))
    def _():
        for i in range(send.shape[0]):
            copy_of(i).wait_send()


def backward_kernel(
    keeps_ref,
    cot_ref,
    held_ref,
    qkv_ref,
    slope_ref,
    mid_ref,
    ln1_gain,
    w_qkv,
    w_proj,
    ln2_gain,
    w_up,
    w_down,
    d_in_ref,
    right_ref,
    small_ref,
    recv,
    send,
    upstream,
    d_heads,
    send_sem,
    recv_sem,
    total_small,
):
    j = pl.program_id(0)
    micro = pl.num_programs(0)
    m = micro - 1 - j
    section = lax.axis_index("section")
    peer = {"section": 1 - section}
    tokens, width = d_in_ref.shape[1:]
    hidden = w_up.shape[1]
    rows = held_ref.shape[1]
    pair = 2 * HEAD_DIM
    scale = HEAD_DIM**-0.5

    @pl.when(j == 0)
    def _():
        meet(peer)
        total_small[...] = jnp.zeros_like(total_small)

    def copy_of(i):
        return pltpu.make_async_remote_copy(
            src_ref=send.at[i],
            dst_ref=recv.at[i],
            send_sem=send_sem.at[i],
            recv_sem=recv_sem.at[i],
            device_id=peer,
            device_id_type=pl.DeviceIdType.MESH,
        )

    @pl.when(section == 1)
    def _():
        fill_rows(upstream, cot_ref)

    @pl.when(section == 0)
    def _():
        copy_of(j).wait_recv()
        upstream[0] = recv[j]

    def add_small(row, values):
        total_small[row : row + 1, :] += jnp.sum(values, axis=0, keepdims=True)

    keep_attn, keep_mlp = (kept(keeps_ref, 0, m), kept(keeps_ref, 1, m))
    d_end = upstream[0].astype(jnp.float32)
    dm_low = (d_end * keep_mlp).astype(jnp.bfloat16)
    first_up = 4 * width
    right_ref[0, :, first_up + hidden : first_up + hidden + width] = dm_low
    parts = hidden // width
    add_small(7 + parts, dm_low.astype(jnp.float32))
    d_c = None
    for part in range(parts):
        span = slice(part * width, (part + 1) * width)
        d_gel = dot_nt(dm_low, w_down[span, :])
        du_low = (d_gel * slope_ref[0, :, span]).astype(jnp.bfloat16)
        right_ref[0, :, first_up + part * width : first_up + (part + 1) * width] = du_low
        add_small(7 + part, du_low.astype(jnp.float32))
        one = dot_nt(du_low, w_up[:, span])
        d_c = one if d_c is None else d_c + one

    def norm_grad(grad, normed, factor, gain, row):
        add_small(row, grad * normed)
        add_small(row + 1, grad)
        scaled = grad * gain
        return factor * (
            scaled
            - jnp.mean(scaled, axis=-1, keepdims=True)
            - normed * jnp.mean(scaled * normed, axis=-1, keepdims=True)
        )

    normed, factor = norm_stats(mid_ref[0])
    d_mid = d_end + norm_grad(d_c, normed, factor, ln2_gain[...], 5)
    dz_low = (d_mid * keep_attn).astype(jnp.bfloat16)
    right_ref[0, :, 3 * width : first_up] = dz_low
    add_small(4, dz_low.astype(jnp.float32))
    d_heads[...] = dot_nt(dz_low, w_proj[...]).astype(jnp.bfloat16)

    masks = head_masks(rows)
    for p in range(width // pair):
        at = [slice(part * width + p * pair, part * width + (p + 1) * pair) for part in range(3)]
        query, keyed, value = (qkv_ref[0, :, span] for span in at)
        d_out = d_heads[:, at[0]]
        grads = [None, None, None]
        for mask in masks:

            def only(x):
                return jnp.where(mask, x, jnp.zeros_like(x))

            query_one, d_one = only(query), only(d_out)
            probs = softmax_rows(query_one * jnp.asarray(scale, jnp.bfloat16), keyed, tokens)
            d_probs = dot_nt(d_one, value)
            inner = jnp.sum(d_probs * probs, axis=-1, keepdims=True)
            ds_low = (probs * (d_probs - inner)).astype(jnp.bfloat16)
            found = (
                dot_nn(ds_low, only(keyed)),
                dot_tn(ds_low, query_one),
                dot_tn(probs.astype(jnp.bfloat16), d_one),
            )
            grads = [f if g is None else g + f for g, f in zip(grads, found)]
        right_ref[0, :, at[0]] = (grads[0] * scale).astype(jnp.bfloat16)
        right_ref[0, :, at[1]] = (grads[1] * scale).astype(jnp.bfloat16)
        right_ref[0, :, at[2]] = grads[2].astype(jnp.bfloat16)

    add_small(2, right_ref[0, :, 0:width].astype(jnp.float32))
    add_small(3, right_ref[0, :, 2 * width : 3 * width].astype(jnp.float32))
    d_a = dot_nt(right_ref[0, :, 0 : 3 * width], w_qkv[...])
    normed, factor = norm_stats(held_ref[0].astype(jnp.float32))
    d_in = d_mid + norm_grad(d_a, normed, factor, ln1_gain[...], 0)
    d_low = d_in.astype(jnp.bfloat16)
    d_in_ref[0] = d_low[0:tokens]

    @pl.when(section == 1)
    def _():
        send[j] = d_low
        copy_of(j).start()

    @pl.when(j == micro - 1)
    def _():
        lines = width // COLS
        for row in range(total_small.shape[0]):
            for i in range(lines):
                small_ref[row * lines + i : row * lines + i + 1, :] = total_small[
                    row : row + 1, i * COLS : (i + 1) * COLS
                ]

    @pl.when((section == 1) & (j == micro - 1))
    def _():
        for i in range(send.shape[0]):
            copy_of(i).wait_send()


def run_layers(inputs, cotangent, weights, keeps):
    (
        gain_one, shift_one, w_qkv, bias_qv, w_proj, b_proj,
        gain_two, shift_two, w_up, b_up, w_down, b_down,
    ) = (w.reshape(1, -1) if w.ndim == 1 else w for w in weights)
    micro, _, tokens, width = inputs.shape
    hidden = w_up.shape[1]
    rows = tokens + -tokens % 16
    low, dma = (jnp.bfloat16, pltpu.SemaphoreType.DMA)

    def fixed(x):
        return pl.BlockSpec(x.shape, lambda i: (0,) * x.ndim, pipeline_mode=pl.Buffered(1))

    def per_step(order, *dims):
        return pl.BlockSpec((1,) + dims, lambda i: (order(i),) + (0,) * len(dims))

    def ahead(i):
        return i

    def back(i):
        return micro - 1 - i

    def params(which):
        return pltpu.CompilerParams(
            collective_id=which,
            has_side_effects=True,
            dimension_semantics=("arbitrary",),
            vmem_limit_bytes=60 * 1024 * 1024,
        )

    smem = pl.BlockSpec(memory_space=pltpu.SMEM)
    big = (w_qkv, w_proj, w_up, w_down)
    loads = [pltpu.VMEM(w.shape, low) for w in big] + [dma((len(big),))]

    def weight(x):
        return pl.BlockSpec(memory_space=pl.ANY) if any(x is w for w in big) else fixed(x)

    consts = (
        gain_one, shift_one, w_qkv, bias_qv, w_proj, b_proj,
        gain_two, shift_two, w_up, b_up, w_down, b_down,
    )
    lefts_width = 3 * width + hidden
    rights_width = 5 * width + hidden
    outputs, held, lefts, qkv, slope, mid = pl.pallas_call(
        forward_kernel,
        grid=(micro,),
        out_shape=(
            jax.ShapeDtypeStruct((micro, tokens, width), low),
            jax.ShapeDtypeStruct((micro, rows, width), low),
            jax.ShapeDtypeStruct((micro, rows, lefts_width), low),
            jax.ShapeDtypeStruct((micro, rows, 3 * width), low),
            jax.ShapeDtypeStruct((micro, rows, hidden), jnp.float32),
            jax.ShapeDtypeStruct((micro, rows, width), jnp.float32),
        ),
        in_specs=[smem, per_step(ahead, 1, tokens, width)] + [weight(x) for x in consts],
        out_specs=(
            per_step(ahead, tokens, width),
            per_step(ahead, rows, width),
            per_step(ahead, rows, lefts_width),
            per_step(ahead, rows, 3 * width),
            per_step(ahead, rows, hidden),
            per_step(ahead, rows, width),
        ),
        scratch_shapes=[
            pltpu.VMEM((micro, rows, width), low),
            pltpu.VMEM((micro, rows, width), low),
            dma((micro,)),
            dma((micro,)),
        ]
        + loads,
        compiler_params=params(1),
    )(keeps, inputs, *consts)
    small_rows = 8 + hidden // width
    small_rows += -small_rows % 8
    consts = (gain_one, w_qkv, w_proj, gain_two, w_up, w_down)
    d_inputs, rights, small = pl.pallas_call(
        backward_kernel,
        grid=(micro,),
        out_shape=(
            jax.ShapeDtypeStruct((micro, tokens, width), low),
            jax.ShapeDtypeStruct((micro, rows, rights_width), low),
            jax.ShapeDtypeStruct((small_rows * width // COLS, COLS), jnp.float32),
        ),
        in_specs=[
            smem,
            per_step(back, 1, tokens, width),
            per_step(back, rows, width),
            per_step(back, rows, 3 * width),
            per_step(back, rows, hidden),
            per_step(back, rows, width),
        ]
        + [fixed(x) for x in consts],
        out_specs=(
            per_step(back, tokens, width),
            per_step(back, rows, rights_width),
            pl.BlockSpec((small_rows * width // COLS, COLS), lambda i: (0, 0)),
        ),
        scratch_shapes=[
            pltpu.VMEM((micro, rows, width), low),
            pltpu.VMEM((micro, rows, width), low),
            pltpu.VMEM((1, rows, width), low),
            pltpu.VMEM((rows, width), low),
            dma((micro,)),
            dma((micro,)),
            pltpu.VMEM((small_rows, width), jnp.float32),
        ],
        compiler_params=params(2),
    )(keeps, cotangent, held, qkv, slope, mid, *consts)
    return (
        outputs,
        d_inputs,
        lefts.reshape(micro * rows, lefts_width),
        rights.reshape(micro * rows, rights_width),
        small,
    )


COLS = 256
SLOTS = 16
PARTIALS = 8


DELAYS = (0, 1, 3, 5, 7, 9, 11, 13, 14, 15)
HOPS = 14


def reduce_kernel(
    count,
    width,
    hidden,
    left_hbm,
    right_hbm,
    small_ref,
    qkv_ref,
    proj_ref,
    up_ref,
    down_ref,
    small_out,
    partial,
    give_core,
    take_core,
    give_ax,
    take_ax,
    give_be,
    take_be,
    give_ae,
    take_ae,
    give_bm,
    take_bm,
    give_am,
    take_am,
    give_bx,
    take_bx,
    whole,
    send_sem,
    recv_sem,
    out_sem,
    left_ref,
    right_ref,
    left_sem,
    right_sem,
):
    per = width // COLS
    first_proj, first_up = (3 * per, 4 * per)
    first_down = first_up + hidden // COLS
    chunks = first_down + per * (hidden // width)
    me = lax.axis_index("dp")
    core = lax.rem(me, 2)
    across = lax.rem(me // 2, 2)
    along = me // 4
    side = along // 2
    at_end = (along == 0) | (along == 3)
    at_middle = (along == 1) | (along == 2)

    def device(z, x, k):
        return {"dp": (z * 2 + x) * 2 + k}

    other_core = device(along, across, 1 - core)
    other_x = device(along, 1 - across, core)
    other_pair = device(along + 1 - 2 * lax.rem(along, 2), across, core)
    other_middle = device(3 - along, across, core)

    def load(src, dst, sem, block):
        columns = pl.ds(pl.multiple_of(block * width, width), width)
        return pltpu.make_async_copy(src.at[:, columns], dst.at[:, columns], sem.at[block])

    def load_left(block):
        return load(left_hbm, left_ref, left_sem, block)

    def load_right(block):
        return load(right_hbm, right_ref, right_sem, block)

    downs = hidden // width
    lefts_of = [0] * 3 + [1] + [2] * downs + list(range(3, 3 + downs))
    rights_of = list(range(4 + downs)) + [4 + downs] * downs
    for i, (left, right) in enumerate(zip(lefts_of, rights_of)):
        if left not in lefts_of[:i]:
            load_left(left).start()
        if right not in rights_of[:i]:
            load_right(right).start()

    barrier = pltpu.get_barrier_semaphore()
    for peer in (other_core, other_x, other_pair, other_middle):
        pl.semaphore_signal(barrier, inc=1, device_id=peer, device_id_type=pl.DeviceIdType.MESH)
    pl.semaphore_wait(barrier, 4)

    lanes_a, lanes_b = (pl.ds(0, COLS // 2), pl.ds(COLS // 2, COLS // 2))
    half = core * 8
    a_part, a_other = (half + across * 4, half + (1 - across) * 4)
    a_mine, a_theirs = (a_part + side * 2, a_part + (1 - side) * 2)
    b_part, b_other = (half + side * 4, half + (1 - side) * 4)
    b_mine, b_theirs = (b_part + across * 2, b_part + (1 - across) * 2)

    def hop(number, src, dst, peer):
        def at(s):
            return pltpu.make_async_remote_copy(
                src_ref=src(s),
                dst_ref=dst(s),
                send_sem=send_sem.at[number, s],
                recv_sem=recv_sem.at[number, s],
                device_id=peer,
                device_id_type=pl.DeviceIdType.MESH,
            )

        return at

    def slot_of(ref):
        return lambda s: ref.at[s]

    def pieces(start, size, lanes=None):
        if lanes is None:
            return lambda s: whole.at[s, pl.ds(start, size)]
        return lambda s: whole.at[s, pl.ds(start, size), :, lanes]

    def spread(number, part, peer):
        return hop(number, part, part, peer)

    core_hop = hop(0, slot_of(give_core), slot_of(take_core), other_core)
    ax_hop = hop(1, slot_of(give_ax), slot_of(take_ax), other_x)
    be_hop = hop(2, slot_of(give_be), slot_of(take_be), other_pair)
    ae_hop = hop(3, slot_of(give_ae), slot_of(take_ae), other_pair)
    bm_hop = hop(4, slot_of(give_bm), slot_of(take_bm), other_middle)
    am_hop = hop(5, slot_of(give_am), slot_of(take_am), other_middle)
    bx_hop = hop(6, slot_of(give_bx), slot_of(take_bx), other_x)
    am_back = spread(7, pieces(a_mine, 2, lanes_a), other_middle)
    bx_back = spread(8, pieces(b_mine, 2, lanes_b), other_x)
    ae_back = spread(9, pieces(a_part, 4, lanes_a), other_pair)
    bm_back = spread(10, pieces(b_part, 4, lanes_b), other_middle)
    ax_back = spread(11, pieces(a_part, 4, lanes_a), other_x)
    be_back = spread(12, pieces(half, 8, lanes_b), other_pair)
    core_back = spread(13, pieces(half, 8), other_core)

    def for_output(u, s, act):
        def go(ref, row, column):
            columns = pl.ds(pl.multiple_of(column * COLS, COLS), COLS)
            dst = ref.at[:, :, columns] if row is None else ref.at[row, :, :, columns]
            act(pltpu.make_async_copy(whole.at[s], dst, out_sem.at[s]))

        @pl.when(u < first_proj)
        def _():
            go(qkv_ref, None, u)

        @pl.when((u >= first_proj) & (u < first_up))
        def _():
            go(proj_ref, None, u - first_proj)

        @pl.when((u >= first_up) & (u < first_down))
        def _():
            go(up_ref, None, u - first_up)

        @pl.when((u >= first_down) & (u < chunks))
        def _():
            go(down_ref, (u - first_down) // per, lax.rem(u - first_down, per))

        @pl.when(u == chunks)
        def _():
            go(small_out, None, 0)

    def low(x):
        return x.astype(jnp.bfloat16)

    def wide(x):
        return x.astype(jnp.float32)

    def products(u, p):
        def reached(k):
            return (u + chunks - k) // chunks

        block = reached(first_proj) + reached(first_up)
        column = u
        for row in range(downs):
            past = reached(first_down + per * row)
            block = block + past
            column = column - per * past if row else column
        fresh = lax.rem(u, per) == 0

        @pl.when((u == 0) | (u == first_proj) | (u == first_up) | (fresh & (u >= first_down)))
        def _():
            load_left(block).wait()

        @pl.when(fresh & (u <= first_down))
        def _():
            load_right(u // per).wait()

        rows = pl.ds(pl.multiple_of(block * width, width), width)
        columns = pl.ds(pl.multiple_of(column * COLS, COLS), COLS)
        product = dot_tn(left_ref[:, rows], right_ref[:, columns])
        partial[p] = product.reshape(partial.shape[1:])

    def add(p, start, size, lanes, found):
        part = (p, pl.ds(start, size), slice(None), lanes)
        total = partial[part] + wide(found)
        partial[part] = total
        return total

    def step(t, carry):
        def stage(number, when=None):
            u = t - DELAYS[number]
            active = (u >= 0) & (u <= chunks)
            if when is not None:
                active = active & when
            s, p = (lax.rem(u + SLOTS, SLOTS), lax.rem(u + SLOTS, PARTIALS))
            return lambda body: pl.when(active)(lambda: body(u, s, p))

        @stage(9)
        def _(u, s, p):
            for_output(u, s, lambda copy: copy.wait())
            for copy in (core_hop, ax_hop, ax_back, core_back):
                copy(s).wait_send()

        @stage(9, at_end)
        def _(u, s, p):
            be_hop(s).wait_send()
            ae_hop(s).wait_send()

        @stage(9, at_middle)
        def _(u, s, p):
            for copy in (bm_hop, am_hop, bx_hop, am_back, bx_back, ae_back, bm_back, be_back):
                copy(s).wait_send()

        @stage(8)
        def _(u, s, p):
            core_back(s).wait_recv()
            for_output(u, s, lambda copy: copy.start())

        @stage(7, at_end)
        def _(u, s, p):
            be_back(s).wait_recv()

        @stage(7)
        def _(u, s, p):
            ax_back(s).wait_recv()
            core_back(s).start()

        @stage(6, at_end)
        def _(u, s, p):
            ae_back(s).wait_recv()

        @stage(6, at_middle)
        def _(u, s, p):
            bm_back(s).wait_recv()
            be_back(s).start()

        @stage(6)
        def _(u, s, p):
            ax_back(s).start()

        @stage(5, at_middle)
        def _(u, s, p):
            am_back(s).wait_recv()
            ae_back(s).start()
            bx_back(s).wait_recv()
            bm_back(s).start()

        @stage(4, at_middle)
        def _(u, s, p):
            am_hop(s).wait_recv()
            mine = pl.ds(a_mine, 2)
            whole[s, mine, :, lanes_a] = low(partial[p, mine, :, lanes_a] + wide(take_am[s]))
            am_back(s).start()
            bx_hop(s).wait_recv()
            mine = pl.ds(b_mine, 2)
            whole[s, mine, :, lanes_b] = low(partial[p, mine, :, lanes_b] + wide(take_bx[s]))
            bx_back(s).start()

        @stage(3, at_middle)
        def _(u, s, p):
            ae_hop(s).wait_recv()
            add(p, a_part, 4, lanes_a, take_ae[s])
            give_am[s] = low(partial[p, pl.ds(a_theirs, 2), :, lanes_a])
            am_hop(s).start()
            bm_hop(s).wait_recv()
            add(p, b_part, 4, lanes_b, take_bm[s])
            give_bx[s] = low(partial[p, pl.ds(b_theirs, 2), :, lanes_b])
            bx_hop(s).start()

        @stage(2)
        def _(u, s, p):
            ax_hop(s).wait_recv()
            total = add(p, a_part, 4, lanes_a, take_ax[s])

            @pl.when(at_end)
            def _():
                give_ae[s] = low(total)
                ae_hop(s).start()

        @stage(2, at_middle)
        def _(u, s, p):
            be_hop(s).wait_recv()
            add(p, half, 8, lanes_b, take_be[s])
            give_bm[s] = low(partial[p, pl.ds(b_other, 4), :, lanes_b])
            bm_hop(s).start()

        @stage(1)
        def _(u, s, p):
            core_hop(s).wait_recv()
            total = add(p, half, 8, slice(None), take_core[s])
            give_ax[s] = low(partial[p, pl.ds(a_other, 4), :, lanes_a])
            ax_hop(s).start()

            @pl.when(at_end)
            def _():
                give_be[s] = low(total[:, :, COLS // 2 :])
                be_hop(s).start()

        @stage(0)
        def _(u, s, p):
            @pl.when(u < chunks)
            def _():
                products(u, p)

            @pl.when(u == chunks)
            def _():
                partial[p] = jnp.zeros(partial.shape[1:], jnp.float32)
                partial[p, 0 : small_ref.shape[0]] = small_ref[...]

            give_core[s] = low(partial[p, pl.ds((1 - core) * 8, 8)])
            core_hop(s).start()

        return carry

    lax.fori_loop(0, chunks + 1 + DELAYS[-1], step, 0)


def sum_weight_grads(lefts, rights, small, width):
    count = lax.axis_size("dp")
    small = small.reshape(-1)
    hidden = rights.shape[1] - 5 * width
    piece = width // count
    if width % COLS or count != 16 or width % (16 * count) or small.size % (piece * COLS) or small.size > width * COLS:
        return sum_weight_grads_plain(lefts, rights, small, width)
    tile = (count, piece, COLS)
    small_in = small.reshape(-1, piece, COLS)
    low, dma = (jnp.bfloat16, pltpu.SemaphoreType.DMA)
    anywhere = pl.BlockSpec(memory_space=pl.ANY)
    vmem = pl.BlockSpec(memory_space=pltpu.VMEM)
    outs = pl.pallas_call(
        functools.partial(reduce_kernel, count, width, hidden),
        out_shape=(
            jax.ShapeDtypeStruct((count, piece, 3 * width), low),
            jax.ShapeDtypeStruct((count, piece, width), low),
            jax.ShapeDtypeStruct((count, piece, hidden), low),
            jax.ShapeDtypeStruct((hidden // width, count, piece, width), low),
            jax.ShapeDtypeStruct(tile, low),
        ),
        in_specs=[anywhere, anywhere, vmem],
        out_specs=(anywhere,) * 5,
        scratch_shapes=[pltpu.VMEM((PARTIALS,) + tile, jnp.float32)]
        + [
            pltpu.VMEM((SLOTS, pieces, piece, lanes), low)
            for pieces, lanes in (
                (8, COLS),
                (4, COLS // 2),
                (8, COLS // 2),
                (4, COLS // 2),
                (4, COLS // 2),
                (2, COLS // 2),
                (2, COLS // 2),
            )
            for _ in range(2)
        ]
        + [
            pltpu.VMEM((SLOTS,) + tile, low),
            dma((HOPS, SLOTS)),
            dma((HOPS, SLOTS)),
            dma((SLOTS,)),
            pltpu.VMEM(lefts.shape, low),
            pltpu.VMEM(rights.shape, low),
            dma((lefts.shape[1] // width,)),
            dma((rights.shape[1] // width,)),
        ],
        compiler_params=pltpu.CompilerParams(
            collective_id=0, has_side_effects=True, vmem_limit_bytes=60 * 1024 * 1024
        ),
    )(lefts, rights, small_in)
    shapes = ((width, 3 * width), (width, width), (width, hidden), (hidden, width))
    sums = [out.reshape(shape) for out, shape in zip(outs[:4], shapes)] + [outs[4]]
    sizes = small_sizes(width, hidden)
    steps = 8

    def band(shape):
        return pl.BlockSpec((shape[0] // steps, shape[1]), lambda i: (i, 0))

    result = pl.pallas_call(
        finish_kernel,
        grid=(steps,),
        out_shape=[jax.ShapeDtypeStruct(shape, jnp.float32) for shape in shapes]
        + [jax.ShapeDtypeStruct((1, size), jnp.float32) for size in sizes],
        in_specs=[band(shape) for shape in shapes] + [pl.BlockSpec(tile, lambda i: (0, 0, 0))],
        out_specs=[band(shape) for shape in shapes]
        + [pl.BlockSpec((1, size), lambda i: (0, 0)) for size in sizes],
        compiler_params=pltpu.CompilerParams(
            dimension_semantics=("arbitrary",), vmem_limit_bytes=48 * 1024 * 1024
        ),
    )(*sums)
    return (result[:4], result[4:])


def small_sizes(width, hidden):
    return (width, width, 2 * width, width, width, width, hidden, width)


def finish_kernel(*refs):
    ins, outs = (refs[:5], refs[5:])
    for src, dst in zip(ins[:4], outs[:4]):
        dst[...] = src[...].astype(jnp.float32)

    @pl.when(pl.program_id(0) == 0)
    def _():
        small, line = (ins[4], 0)
        for dst in outs[4:]:
            for i in range(dst.shape[1] // COLS):
                piece, row = divmod(line, small.shape[1])
                dst[:, i * COLS : (i + 1) * COLS] = small[piece, row : row + 1, :].astype(
                    jnp.float32
                )
                line += 1


def sum_weight_grads_plain(lefts, rights, small, width):
    hidden = rights.shape[1] - 5 * width

    def product(l_start, l_size, r_start, r_size):
        return lax.dot_general(
            lefts[:, l_start : l_start + l_size],
            rights[:, r_start : r_start + r_size],
            (((0,), (0,)), ((), ())),
            preferred_element_type=jnp.float32,
        )

    totals = (
        product(0, width, 0, 3 * width),
        product(width, width, 3 * width, width),
        product(2 * width, width, 4 * width, hidden),
        product(3 * width, hidden, 4 * width + hidden, width),
        jnp.pad(small, (0, -small.size % lax.axis_size("dp"))),
    )
    totals = lax.psum_scatter(totals, "dp", scatter_dimension=0, tiled=True)
    whole = lax.all_gather(as_sent(totals), "dp", axis=0, tiled=True)
    whole = jax.tree.map(lambda part: part.astype(jnp.float32), whole)
    sizes = small_sizes(width, hidden)
    starts = [sum(sizes[:i]) for i in range(len(sizes))]
    parts = [whole[4][None, s : s + size] for s, size in zip(starts, sizes)]
    return (whole[:4], parts)


def per_device(
    inputs,
    ln1_gain,
    ln1_bias,
    qkv_weight,
    qv_bias,
    proj_weight,
    proj_bias,
    ln2_gain,
    ln2_bias,
    fc1_weight,
    fc1_bias,
    fc2_weight,
    fc2_bias,
    keep_masks,
    cotangent,
):
    weights = tuple(
        (
            w[0]
            for w in (
                ln1_gain,
                ln1_bias,
                qkv_weight,
                qv_bias,
                proj_weight,
                proj_bias,
                ln2_gain,
                ln2_bias,
                fc1_weight,
                fc1_bias,
                fc2_weight,
                fc2_bias,
            )
        )
    )
    keeps = keep_masks[0, :, :, 0]
    outputs, d_inputs, lefts, rights, small = run_layers(inputs, cotangent, weights, keeps)
    big, small = sum_weight_grads(lefts, rights, small, inputs.shape[-1])
    qkv, proj, up, down = (x[None] for x in big)
    return (
        outputs[None, :, None],
        d_inputs[None, :, None],
        small[0],
        small[1],
        qkv,
        small[2],
        proj,
        small[3],
        small[4],
        small[5],
        up,
        small[6],
        down,
        small[7],
    )


def solution(mesh):
    in_specs = (
        P(None, "dp", None, None),
        P("section", None),
        P("section", None),
        P("section", None, None),
        P("section", None),
        P("section", None, None),
        P("section", None),
        P("section", None),
        P("section", None),
        P("section", None, None),
        P("section", None),
        P("section", None, None),
        P("section", None),
        P("section", None, None, "dp"),
        P(None, "dp", None, None),
    )
    out_specs = (
        P("section", None, "dp", None, None),
        P("section", None, "dp", None, None),
        P("section", None),
        P("section", None),
        P("section", None, None),
        P("section", None),
        P("section", None, None),
        P("section", None),
        P("section", None),
        P("section", None),
        P("section", None, None),
        P("section", None),
        P("section", None, None),
        P("section", None),
    )
    return jax.shard_map(
        per_device, mesh=mesh, in_specs=in_specs, out_specs=out_specs, check_vma=False
    )
```
